8 devices in a mesh: fsdp: 4 (over z, y, x), model: 2 (over core).
Axes of the slice: x: 2, y: 2, z: 1, core: 2. Of those that a mesh axis runs over, the one named last changes fastest.
Arguments:
- x_in: bfloat16 [32, 1024, 1536], P('fsdp', 'model')
- gain_attn: float32 [2, 1536], replicated
- gain_mlp: float32 [2, 1536], replicated
- rope_cos: float32 [1024, 64], replicated
- rope_sin: float32 [1024, 64], replicated
- w_q: bfloat16 [2, 1536, 1536], P(None, 'fsdp', 'model')
- w_k: bfloat16 [2, 1536, 256], P(None, 'fsdp', 'model')
- w_v: bfloat16 [2, 1536, 256], P(None, 'fsdp', 'model')
- w_o: bfloat16 [2, 1536, 1536], P(None, 'model', 'fsdp')
- w_gate: bfloat16 [2, 1536, 8960], P(None, 'fsdp', 'model')
- w_up: bfloat16 [2, 1536, 8960], P(None, 'fsdp', 'model')
- w_down: bfloat16 [2, 8960, 1536], P(None, 'model', 'fsdp')
Outputs:
- output: bfloat16 [32, 1024, 1536], P('fsdp', 'model')
All inputs are finite; a program needn't handle non-finite values.
Results may differ from the reference program's by a relative error of at most 0.02.
Values are sent between devices in bfloat16 or wider.
A program may use at most 1 GiB of HBM per device.

```python
import math
import jax
import jax.numpy as jnp
from jax import lax

D_MODEL = 1536
FFN = 8960
HEADS = 12
KV_HEADS = 2
HEAD_DIM = 128
BATCH = 32
SEQ = 1024
LAYERS = 2
EPS = 1e-5
ROPE_BASE = 500000.0


def rope_tables(rng_key):
    pos_steps = jax.random.randint(rng_key, (SEQ,), 1, 4)
    positions = (jnp.cumsum(pos_steps) - pos_steps[0]).astype(jnp.float32)
    inv_freq = ROPE_BASE ** (-jnp.arange(HEAD_DIM // 2, dtype=jnp.float32) * (2.0 / HEAD_DIM))
    angles = positions[:, None] * inv_freq[None, :]
    return jnp.cos(angles), jnp.sin(angles)


def setup_inputs(seed: int = 0) -> dict:
    key_list = jax.random.split(jax.random.key(seed), 12)
    q_scale = math.sqrt(max(1.0, math.log(SEQ / 16.0)))

    def normal(rng_key, arr_shape, std_scale):
        return (jax.random.normal(rng_key, arr_shape, jnp.float32) * std_scale).astype(jnp.bfloat16)

    rope_cos, rope_sin = rope_tables(key_list[3])
    return {
        'x_in': normal(key_list[0], (BATCH, SEQ, D_MODEL), 1.0),
        'gain_attn': jax.random.uniform(key_list[1], (LAYERS, D_MODEL), jnp.float32, 0.5, 1.5),
        'gain_mlp': jax.random.uniform(key_list[2], (LAYERS, D_MODEL), jnp.float32, 0.5, 1.5),
        'rope_cos': rope_cos,
        'rope_sin': rope_sin,
        'w_q': normal(key_list[4], (LAYERS, D_MODEL, HEADS * HEAD_DIM), q_scale * D_MODEL ** -0.5),
        'w_k': normal(key_list[5], (LAYERS, D_MODEL, KV_HEADS * HEAD_DIM), D_MODEL ** -0.5),
        'w_v': normal(key_list[6], (LAYERS, D_MODEL, KV_HEADS * HEAD_DIM), D_MODEL ** -0.5),
        'w_o': normal(key_list[7], (LAYERS, HEADS * HEAD_DIM, D_MODEL), 2.0 * (HEADS * HEAD_DIM) ** -0.5),
        'w_gate': normal(key_list[8], (LAYERS, D_MODEL, FFN), D_MODEL ** -0.5),
        'w_up': normal(key_list[9], (LAYERS, D_MODEL, FFN), D_MODEL ** -0.5),
        'w_down': normal(key_list[10], (LAYERS, FFN, D_MODEL), FFN ** -0.5),
    }


def rms_norm(seq_rows, gain_vec):
    rows_f = seq_rows.astype(jnp.float32)
    mean_sq = jnp.mean(rows_f * rows_f, axis=-1, keepdims=True)
    return (rows_f * lax.rsqrt(mean_sq + EPS) * gain_vec).astype(jnp.bfloat16)


def rotate(head_vals, cos_b, sin_b):
    half_dim = head_vals.shape[-1] // 2
    heads_f = head_vals.astype(jnp.float32)
    first_half = heads_f[..., :half_dim]
    second_half = heads_f[..., half_dim:]
    return jnp.concatenate([first_half * cos_b - second_half * sin_b, second_half * cos_b + first_half * sin_b], axis=-1).astype(jnp.bfloat16)


def decoder_layer(seq_rows, params, rope_cos, rope_sin):
    gain_attn, gain_mlp, w_q, w_k, w_v, w_o, w_gate, w_up, w_down = params
    group_size = HEADS // KV_HEADS
    normed = rms_norm(seq_rows, gain_attn)
    q_proj = jnp.dot(normed, w_q, preferred_element_type=jnp.float32).astype(jnp.bfloat16).reshape(SEQ, KV_HEADS, group_size, HEAD_DIM)
    k_proj = jnp.dot(normed, w_k, preferred_element_type=jnp.float32).astype(jnp.bfloat16).reshape(SEQ, KV_HEADS, HEAD_DIM)
    v_proj = jnp.dot(normed, w_v, preferred_element_type=jnp.float32).astype(jnp.bfloat16).reshape(SEQ, KV_HEADS, HEAD_DIM)
    q_rot = rotate(q_proj, rope_cos[:, None, None, :], rope_sin[:, None, None, :])
    k_rot = rotate(k_proj, rope_cos[:, None, :], rope_sin[:, None, :])
    scores = jnp.einsum('qkgd,skd->kgqs', q_rot.astype(jnp.float32), k_rot.astype(jnp.float32)) * HEAD_DIM ** -0.5
    positions = jnp.arange(SEQ)
    causal = positions[:, None] >= positions[None, :]
    scores = jnp.where(causal, scores, -jnp.inf)
    attn_probs = jax.nn.softmax(scores, axis=-1).astype(jnp.bfloat16)
    attn_out = jnp.einsum('kgqs,skd->qkgd', attn_probs.astype(jnp.float32), v_proj.astype(jnp.float32)).astype(jnp.bfloat16).reshape(SEQ, HEADS * HEAD_DIM)
    attn_sum = jnp.dot(attn_out, w_o, preferred_element_type=jnp.float32)
    mid_rows = (seq_rows.astype(jnp.float32) + attn_sum).astype(jnp.bfloat16)
    normed_mlp = rms_norm(mid_rows, gain_mlp)
    gate_acc = jnp.dot(normed_mlp, w_gate, preferred_element_type=jnp.float32)
    up_acc = jnp.dot(normed_mlp, w_up, preferred_element_type=jnp.float32)
    hidden = (jax.nn.silu(gate_acc) * up_acc).astype(jnp.bfloat16)
    mlp_sum = jnp.dot(hidden, w_down, preferred_element_type=jnp.float32)
    return (mid_rows.astype(jnp.float32) + mlp_sum).astype(jnp.bfloat16)


def reference(x_in, gain_attn, gain_mlp, rope_cos, rope_sin, w_q, w_k, w_v, w_o, w_gate, w_up, w_down):
    params = (gain_attn, gain_mlp, w_q, w_k, w_v, w_o, w_gate, w_up, w_down)

    def one_sequence(seq_rows):
        def layer_step(carry_rows, layer_params):
            return decoder_layer(carry_rows, layer_params, rope_cos, rope_sin), None
        final_rows, _ = lax.scan(layer_step, seq_rows, params)
        return final_rows

    return lax.map(one_sequence, x_in)
```

```python
import functools
import math

import jax
import jax.numpy as jnp
from jax import lax
from jax.experimental import pallas as pl
from jax.experimental.pallas import tpu as pltpu
from jax.sharding import PartitionSpec as P

EPS = 1e-5
HEAD_DIM = 128
TILE_Q = 256


def norm_kernel(x_ref, g_ref, o_ref):
    rows = x_ref[...].astype(jnp.float32)
    mean_sq = jnp.mean(rows * rows, axis=-1, keepdims=True)
    o_ref[...] = (rows * lax.rsqrt(mean_sq + EPS) * g_ref[...]).astype(jnp.bfloat16)


def rms_norm(x, gain):
    rows, width = x.shape
    tile = 512
    return pl.pallas_call(
        norm_kernel,
        grid=(rows // tile,),
        in_specs=[pl.BlockSpec((tile, width), lambda i: (i, 0)), pl.BlockSpec((1, width), lambda i: (0, 0))],
        out_specs=pl.BlockSpec((tile, width), lambda i: (i, 0)),
        out_shape=jax.ShapeDtypeStruct((rows, width), jnp.bfloat16),
        compiler_params=pltpu.CompilerParams(dimension_semantics=("arbitrary",), vmem_limit_bytes=60 << 20),
        cost_estimate=pl.CostEstimate(flops=rows * width * 8, bytes_accessed=rows * width * 4, transcendentals=rows),
        name="rms_norm",
    )(x, gain[None, :])


def attn_kernel(heads, qkv_ref, cos_ref, sin_ref, o_ref, k_ref):
    seq = qkv_ref.shape[0]
    half = HEAD_DIM // 2
    factor = HEAD_DIM ** -0.5 * math.log2(math.e)
    k_col = heads * HEAD_DIM

    def rotary(vals, rows):
        vals = vals.astype(jnp.float32)
        return (vals * cos_ref[rows, :] + pltpu.roll(vals, half, 1) * sin_ref[rows, :]).astype(jnp.bfloat16)

    for i in range(seq // TILE_Q):
        rows = pl.ds(i * TILE_Q, TILE_Q)
        k_ref[rows, :] = rotary(qkv_ref[rows, pl.ds(k_col, HEAD_DIM)], rows)
    row_id = lax.broadcasted_iota(jnp.int32, (TILE_Q, TILE_Q), 0)
    col_id = lax.broadcasted_iota(jnp.int32, (TILE_Q, TILE_Q), 1)
    causal = row_id >= col_id

    @pl.loop(0, heads)
    def _(head):
        cols = pl.ds(pl.multiple_of(head * HEAD_DIM, HEAD_DIM), HEAD_DIM)
        for i in range(seq // TILE_Q):
            rows = pl.ds(i * TILE_Q, TILE_Q)
            keys = (i + 1) * TILE_Q
            q = rotary(qkv_ref[rows, cols], rows)
            s = lax.dot_general(q, k_ref[:keys, :], (((1,), (1,)), ((), ())), preferred_element_type=jnp.float32)
            diag = jnp.where(causal, s[:, keys - TILE_Q:], -jnp.inf)
            s = jnp.concatenate([s[:, :keys - TILE_Q], diag], axis=1) if i else diag
            top = jnp.max(s, axis=1, keepdims=True)
            e = jnp.exp2((s - top) * factor)
            p = (e * (1.0 / jnp.sum(e, axis=1, keepdims=True))).astype(jnp.bfloat16)
            v = qkv_ref[:keys, k_col + HEAD_DIM:k_col + 2 * HEAD_DIM]
            o_ref[rows, cols] = jnp.dot(p, v, preferred_element_type=jnp.float32).astype(jnp.bfloat16)


def attention(qkv, cos, sin, seq):
    tokens, width = qkv.shape
    heads = width // HEAD_DIM - 2
    table = pl.BlockSpec((seq, HEAD_DIM), lambda b: (0, 0))
    return pl.pallas_call(
        functools.partial(attn_kernel, heads),
        grid=(tokens // seq,),
        in_specs=[pl.BlockSpec((seq, width), lambda b: (b, 0)), table, table],
        out_specs=pl.BlockSpec((seq, heads * HEAD_DIM), lambda b: (b, 0)),
        out_shape=jax.ShapeDtypeStruct((tokens, heads * HEAD_DIM), jnp.bfloat16),
        scratch_shapes=[pltpu.VMEM((seq, HEAD_DIM), jnp.bfloat16)],
        compiler_params=pltpu.CompilerParams(dimension_semantics=("arbitrary",), vmem_limit_bytes=60 << 20),
        cost_estimate=pl.CostEstimate(flops=tokens * heads * seq * HEAD_DIM * 4, bytes_accessed=tokens * width * 4, transcendentals=tokens * heads * seq // 2),
        name="attend",
    )(qkv, cos, sin)


def mm(a, b):
    return jnp.dot(a, b, preferred_element_type=jnp.float32)


def solution(mesh):
    act_spec = P('fsdp', 'model', None)
    col_spec = P(None, 'fsdp', 'model')
    row_spec = P(None, 'model', 'fsdp')
    swap = [(0, 1), (1, 0)]

    def gather(block, axis):
        return lax.all_gather(block, 'fsdp', axis=axis, tiled=True)

    def after(value, token):
        return lax.optimization_barrier((value, token))[0]

    def pair(own, token=None):
        own = own if token is None else after(own, token)
        return own, lax.ppermute(own, 'model', swap)

    def device_step(x_in, gain_attn, gain_mlp, rope_cos, rope_sin, w_q, w_k, w_v, w_o, w_gate, w_up, w_down):
        layers = w_q.shape[0]
        cos = jnp.concatenate([rope_cos, rope_cos], axis=1)
        sin = jnp.concatenate([-rope_sin, rope_sin], axis=1)
        own = []
        for l in range(layers):
            qkv = gather(jnp.concatenate([w_q[l], w_k[l], w_v[l]], axis=1), 0)
            own.append((qkv, gather(w_o[l], 1), gather(w_gate[l], 0), gather(w_up[l], 0), gather(w_down[l], 1)))
        x = lax.all_to_all(x_in, 'model', split_axis=0, concat_axis=1, tiled=True)
        batch, seq, width = x.shape
        x = x.reshape(batch * seq, width)
        qkv_w = pair(own[0][0])
        for l in range(layers):
            early = l > 0
            h = rms_norm(x, gain_attn[l])
            qkv0 = mm(h, qkv_w[0]).astype(jnp.bfloat16)
            o_w = pair(own[l][1], qkv0)
            o0 = attention(qkv0, cos, sin, seq)
            qkv1 = mm(h, qkv_w[1]).astype(jnp.bfloat16)
            if early:
                gate_w = pair(own[l][2], o0)
            o1 = attention(qkv1, cos, sin, seq)
            part = mm(o0, o_w[0])
            m = (x.astype(jnp.float32) + (part + mm(o1, o_w[1]))).astype(jnp.bfloat16)
            u = rms_norm(m, gain_mlp[l])
            if not early:
                gate_w = pair(own[l][2], u)
            gate0 = mm(u, gate_w[0])
            if early:
                up_w = pair(own[l][3], gate0)
            gate1 = mm(u, gate_w[1])
            if not early:
                up_w = pair(own[l][3], gate1)
            if early:
                up_w = (after(up_w[0], gate1), up_w[1])
            z0 = lax.optimization_barrier((jax.nn.silu(gate0) * mm(u, up_w[0])).astype(jnp.bfloat16))
            if early:
                down_w = pair(own[l][4], z0)
            z1 = lax.optimization_barrier((jax.nn.silu(gate1) * mm(u, up_w[1])).astype(jnp.bfloat16))
            if not early:
                down_w = pair(own[l][4], z1)
            if early:
                down_w = (after(down_w[0], z1), down_w[1])
            part = mm(z0, down_w[0])
            if l + 1 < layers:
                qkv_w = pair(own[l + 1][0], part)
            x = (m.astype(jnp.float32) + (part + mm(z1, down_w[1]))).astype(jnp.bfloat16)
        return lax.all_to_all(x.reshape(batch, seq, width), 'model', split_axis=1, concat_axis=0, tiled=True)

    return jax.shard_map(device_step, mesh=mesh, in_specs=(act_spec, P(), P(), P(), P(), col_spec, col_spec, col_spec, row_spec, col_spec, col_spec, row_spec), out_specs=act_spec, check_vma=False)
```

```python
import functools
import math

import jax
import jax.numpy as jnp
from jax import lax
from jax.experimental import pallas as pl
from jax.experimental.pallas import tpu as pltpu
from jax.sharding import PartitionSpec as P

EPS = 1e-5
HEAD_DIM = 128
TILE_Q = 256
PIECE = 640
SPLIT = 4
SLOTS = 2
VMEM_LIMIT = 62 << 20


def params(limit=VMEM_LIMIT, axes=1):
    return pltpu.CompilerParams(dimension_semantics=("arbitrary",) * axes, vmem_limit_bytes=limit)


def cost(flops, data, exps=0):
    return pl.CostEstimate(flops=flops, bytes_accessed=data, transcendentals=exps)


def mm(a, b):
    return jnp.dot(a, b, preferred_element_type=jnp.float32)


def normalize(rows, gain):
    mean_sq = jnp.mean(rows * rows, axis=-1, keepdims=True)
    return (rows * lax.rsqrt(mean_sq + EPS) * gain).astype(jnp.bfloat16)


def resident(shape):
    return pl.BlockSpec(shape, lambda *i: (0,) * len(shape), pipeline_mode=pl.Buffered(1))


def norm_kernel(x_ref, g_ref, o_ref):
    for r in range(0, x_ref.shape[0], 128):
        rows = pl.ds(r, 128)
        o_ref[rows, :] = normalize(x_ref[rows, :].astype(jnp.float32), g_ref[...])


def norm(x, gain, tile, order):
    rows, width = x.shape
    return pl.pallas_call(
        norm_kernel,
        grid=(rows // tile,),
        in_specs=[pl.BlockSpec((tile, width), lambda i: (order(i), 0)), resident((1, width))],
        out_specs=pl.BlockSpec((tile, width), lambda i: (i, 0)),
        out_shape=jax.ShapeDtypeStruct((rows, width), jnp.bfloat16),
        compiler_params=params(),
        cost_estimate=cost(rows * width * 8, rows * width * 4),
        name="norm",
    )(x, gain)


def attn_kernel(heads, h_ref, w_ref, cos_ref, sin_ref, o_ref, qkv_ref, vt_ref, s_ref):
    seq = h_ref.shape[0]
    half = HEAD_DIM // 2
    factor = HEAD_DIM ** -0.5 * math.log2(math.e)
    k_col = heads * HEAD_DIM
    v_col = k_col + HEAD_DIM
    tiles = seq // TILE_Q

    for c in range(0, w_ref.shape[1], 256):
        qkv_ref[:, c:c + 256] = mm(h_ref[...], w_ref[:, c:c + 256]).astype(jnp.bfloat16)

    def rotary(vals, rows):
        vals = vals.astype(jnp.float32)
        return (vals * cos_ref[rows, :] + pltpu.roll(vals, half, 1) * sin_ref[rows, :]).astype(jnp.bfloat16)

    for i in range(tiles):
        rows = pl.ds(i * TILE_Q, TILE_Q)
        qkv_ref[rows, k_col:v_col] = rotary(qkv_ref[rows, k_col:v_col], rows)
        vt_ref[:, i * TILE_Q:(i + 1) * TILE_Q] = qkv_ref[rows, v_col:v_col + HEAD_DIM].astype(jnp.float32).T.astype(jnp.bfloat16)
    key_id = lax.broadcasted_iota(jnp.int32, (TILE_Q, TILE_Q), 0)
    query_id = lax.broadcasted_iota(jnp.int32, (TILE_Q, TILE_Q), 1)
    causal = query_id >= key_id
    groups = (TILE_Q // 8, 8, TILE_Q)

    def scores(head, slot, i):
        cols = pl.ds(pl.multiple_of(head * HEAD_DIM, HEAD_DIM), HEAD_DIM)
        rows = pl.ds(i * TILE_Q, TILE_Q)
        q = rotary(qkv_ref[rows, cols], rows)
        top = None
        for j in range(i + 1):
            keys = pl.ds(j * TILE_Q, TILE_Q)
            s = lax.dot_general(qkv_ref[keys, k_col:v_col], q, (((1,), (1,)), ((), ())), preferred_element_type=jnp.float32)
            if i == j:
                s = jnp.where(causal, s, -jnp.inf)
            s_ref[slot, i, keys, :] = s
            part = jnp.max(s.reshape(groups), axis=0)
            top = part if top is None else jnp.maximum(top, part)
        return jnp.max(top, axis=0, keepdims=True)

    def powers(slot, i, top):
        total = None
        for j in range(i + 1):
            keys = pl.ds(j * TILE_Q, TILE_Q)
            e = jnp.exp2((s_ref[slot, i, keys, :] - top) * factor)
            s_ref[slot, i, keys, :] = e
            part = jnp.sum(e.reshape(groups), axis=0)
            total = part if total is None else total + part
        return 1.0 / jnp.sum(total, axis=0, keepdims=True)

    def values(head, slot, i, inverse):
        cols = pl.ds(pl.multiple_of(head * HEAD_DIM, HEAD_DIM), HEAD_DIM)
        keys = (i + 1) * TILE_Q
        p = (s_ref[slot, i, :keys, :] * inverse).astype(jnp.bfloat16)
        o_ref[pl.ds(i * TILE_Q, TILE_Q), cols] = mm(vt_ref[:, :keys], p).T.astype(jnp.bfloat16)

    @pl.loop(0, heads // SLOTS)
    def _(step):
        work = [(step * SLOTS + slot, slot, i) for slot in range(SLOTS) for i in reversed(range(tiles))]
        tops, inverses = {}, {}
        for t in range(len(work) + 2):
            if t < len(work):
                tops[t] = scores(*work[t])
            if 0 <= t - 1 < len(work):
                inverses[t - 1] = powers(*work[t - 1][1:], tops[t - 1])
            if 0 <= t - 2 < len(work):
                values(*work[t - 2], inverses[t - 2])


def attention(h, w, cos, sin, seq):
    tokens, depth = h.shape
    width = w.shape[1]
    heads = width // HEAD_DIM - 2
    return pl.pallas_call(
        functools.partial(attn_kernel, heads),
        grid=(tokens // seq,),
        in_specs=[pl.BlockSpec((seq, depth), lambda b: (b, 0)), resident(w.shape), resident(cos.shape), resident(sin.shape)],
        out_specs=pl.BlockSpec((seq, heads * HEAD_DIM), lambda b: (b, 0)),
        out_shape=jax.ShapeDtypeStruct((tokens, heads * HEAD_DIM), jnp.bfloat16),
        scratch_shapes=[
            pltpu.VMEM((seq, width), jnp.bfloat16),
            pltpu.VMEM((HEAD_DIM, seq), jnp.bfloat16),
            pltpu.VMEM((SLOTS, seq // TILE_Q, seq, TILE_Q), jnp.float32),
        ],
        compiler_params=params(),
        cost_estimate=cost(2 * tokens * depth * width + tokens * heads * seq * HEAD_DIM * 4, tokens * width * 4, tokens * heads * seq // 2),
        name="attend",
    )(h, w, cos, sin)


def out_kernel(a_ref, b_ref, wa_ref, wb_ref, x_ref, g_ref, m_ref, u_ref):
    for r in range(0, a_ref.shape[0], 256):
        rows = pl.ds(r, 256)
        acc = mm(a_ref[rows, :], wa_ref[...]) + mm(b_ref[rows, :], wb_ref[...])
        m = (x_ref[rows, :].astype(jnp.float32) + acc).astype(jnp.bfloat16)
        m_ref[rows, :] = m
        u_ref[rows, :] = normalize(m.astype(jnp.float32), g_ref[...])


def out_product(a, b, wa, wb, x, gain, order):
    tokens, depth = a.shape
    width = wa.shape[1]
    tile = 512
    lhs = pl.BlockSpec((tile, depth), lambda i: (i, 0))
    out = pl.BlockSpec((tile, width), lambda i: (i, 0))
    shape = jax.ShapeDtypeStruct((tokens, width), jnp.bfloat16)
    return pl.pallas_call(
        out_kernel,
        grid=(tokens // tile,),
        in_specs=[lhs, lhs, resident(wa.shape), resident(wb.shape), pl.BlockSpec((tile, width), lambda i: (order(i), 0)), resident((1, width))],
        out_specs=[out, out],
        out_shape=[shape, shape],
        compiler_params=params(),
        cost_estimate=cost(4 * tokens * depth * width, tokens * width * 10),
        name="out_product",
    )(a, b, wa, wb, x, gain)


def glu_kernel(u_ref, g_ref, v_ref, z_ref):
    for c in range(0, z_ref.shape[1], 128):
        cols = slice(c, c + 128)
        both = mm(u_ref[...], jnp.concatenate([g_ref[:, cols], v_ref[:, cols]], axis=1))
        z_ref[:, cols] = (jax.nn.silu(both[:, :128]) * both[:, 128:]).astype(jnp.bfloat16)


def glu(u, w):
    tokens, depth = u.shape
    width = w.shape[1] // 2
    tile, steps = 1024, width // PIECE
    return pl.pallas_call(
        glu_kernel,
        grid=(tokens // tile, steps),
        in_specs=[
            pl.BlockSpec((tile, depth), lambda i, j: (i, 0)),
            pl.BlockSpec((depth, PIECE), lambda i, j: (0, j)),
            pl.BlockSpec((depth, PIECE), lambda i, j: (0, j + steps)),
        ],
        out_specs=pl.BlockSpec((tile, PIECE), lambda i, j: (i, j)),
        out_shape=jax.ShapeDtypeStruct((tokens, width), jnp.bfloat16),
        compiler_params=params(axes=2),
        cost_estimate=cost(4 * tokens * depth * width, tokens * width * 2 + depth * width * 16, tokens * width),
        name="glu",
    )(u, w, w)


def down_sum(a_ref, b_ref, w_ref):
    cut = a_ref.shape[1]
    return mm(a_ref[...], w_ref[:cut, :]) + mm(b_ref[...], w_ref[cut:, :])


def first_kernel(a_ref, b_ref, w_ref, o_ref):
    o_ref[...] = down_sum(a_ref, b_ref, w_ref)


def second_kernel(a_ref, b_ref, w_ref, p_ref, m_ref, g_ref, x_ref, h_ref=None):
    x = (m_ref[...].astype(jnp.float32) + (p_ref[...] + down_sum(a_ref, b_ref, w_ref))).astype(jnp.bfloat16)
    x_ref[...] = x
    if h_ref is not None:
        h_ref[...] = normalize(x.astype(jnp.float32), g_ref[...])


def down_product(a, b, w, rest=None, last=False, order=lambda i: i):
    tokens = a.shape[0]
    depth, width = w.shape
    tile = 256
    row = lambda n: pl.BlockSpec((tile, n), lambda i: (i, 0))
    in_specs = [row(a.shape[1]), row(b.shape[1]), resident(w.shape)]
    shape = lambda kind: jax.ShapeDtypeStruct((tokens, width), kind)
    if rest is None:
        kernel, rest, out_specs, out_shape = first_kernel, (), row(width), shape(jnp.float32)
    else:
        kernel = second_kernel
        in_specs += [row(width), row(width), resident((1, width))]
        x_spec = pl.BlockSpec((tile, width), lambda i: (order(i), 0))
        out_specs = [x_spec] if last else [x_spec, row(width)]
        out_shape = [shape(jnp.bfloat16)] * len(out_specs)
    return pl.pallas_call(
        kernel,
        grid=(tokens // tile,),
        in_specs=in_specs,
        out_specs=out_specs,
        out_shape=out_shape,
        compiler_params=params(),
        cost_estimate=cost(2 * tokens * depth * width, tokens * (depth * 2 + width * 8)),
        name="down_product",
    )(a, b, w, *rest)


def solution(mesh):
    act_spec = P('fsdp', 'model', None)
    col_spec = P(None, 'fsdp', 'model')
    row_spec = P(None, 'model', 'fsdp')
    swap = [(0, 1), (1, 0)]

    def gather(block, axis):
        return lax.all_gather(block, 'fsdp', axis=axis, tiled=True)

    def after(value, token):
        return lax.optimization_barrier((value, token))[0]

    def pair(own, token=None):
        own = own if token is None else after(own, token)
        return own, lax.ppermute(own, 'model', swap)

    def exchange(x):
        return lax.all_to_all(x, 'model', split_axis=0, concat_axis=0, tiled=True)

    def device_step(x_in, gain_attn, gain_mlp, rope_cos, rope_sin, w_q, w_k, w_v, w_o, w_gate, w_up, w_down):
        layers = w_q.shape[0]
        batch, part, width = x_in.shape
        seqs, seq = batch // 2, 2 * part
        cos = jnp.concatenate([rope_cos, rope_cos], axis=1)
        sin = jnp.concatenate([-rope_sin, rope_sin], axis=1)
        cut = SPLIT * PIECE

        def weave(tile):
            per = part // tile

            def order(i):
                b, r = i // (2 * per), i % (2 * per)
                return (r // per) * (seqs * per) + b * per + r % per
            return order

        own = []
        for l in range(layers):
            qkv = gather(jnp.concatenate([w_q[l], w_k[l], w_v[l]], axis=1), 0)
            w_out = gather(w_o[l], 1)
            gu_a = gather(jnp.concatenate([w_gate[l][:, :cut], w_up[l][:, :cut]], axis=1), 0)
            gu_b = gather(jnp.concatenate([w_gate[l][:, cut:], w_up[l][:, cut:]], axis=1), 0)
            own.append((qkv, w_out, gu_a, gu_b, gather(w_down[l], 1)))
        x = exchange(x_in).reshape(batch * part, width)
        h = norm(x, gain_attn[0][None], 512, weave(512))
        for l, (qkv_own, o_own, a_own, b_own, d_own) in enumerate(own):
            qkv_w = pair(qkv_own, h)
            o0 = attention(h, qkv_w[0], cos, sin, seq)
            o_w = pair(o_own, o0)
            o1 = attention(h, qkv_w[1], cos, sin, seq)
            m, u = out_product(o0, o1, o_w[0], o_w[1], x, gain_mlp[l][None], weave(512) if l == 0 else lambda i: i)
            a_w = pair(a_own, u)
            za = [glu(u, a_w[0])]
            za.append(glu(after(u, za[0]), a_w[1]))
            b_w = pair(b_own, za[1])
            zb = [glu(u, b_w[0])]
            zb.append(glu(after(u, zb[0]), b_w[1]))
            d_w = pair(d_own, zb[1])
            partial = down_product(za[0], zb[0], d_w[0])
            last = l + 1 == layers
            gain = gain_attn[0 if last else l + 1][None]
            out = down_product(za[1], zb[1], d_w[1], (partial, m, gain), last, weave(256) if last else lambda i: i)
            x, h = out if not last else (out[0], None)
        return exchange(x.reshape(batch, part, width))

    return jax.shard_map(device_step, mesh=mesh, in_specs=(act_spec, P(), P(), P(), P(), col_spec, col_spec, col_spec, row_spec, col_spec, col_spec, row_spec), out_specs=act_spec, check_vma=False)
```

```python
import functools
import math

import jax
import jax.numpy as jnp
from jax import lax
from jax.experimental import pallas as pl
from jax.experimental.pallas import tpu as pltpu
from jax.sharding import PartitionSpec as P

EPS = 1e-5
HEAD_DIM = 128
TILE_Q = 256
PIECE = 640
SPLIT = 4
SLOTS = 2
GLU_ROWS = 512
DOWN_ROWS = 256
OUT_ROWS = 256
VMEM_LIMIT = 62 << 20


def params(limit=VMEM_LIMIT, axes=1):
    return pltpu.CompilerParams(dimension_semantics=("arbitrary",) * axes, vmem_limit_bytes=limit)


def cost(flops, data, exps=0):
    return pl.CostEstimate(flops=flops, bytes_accessed=data, transcendentals=exps)


def mm(a, b):
    return jnp.dot(a, b, preferred_element_type=jnp.float32)


def normalize(rows, gain):
    mean_sq = jnp.mean(rows * rows, axis=-1, keepdims=True)
    return (rows * lax.rsqrt(mean_sq + EPS) * gain).astype(jnp.bfloat16)


def resident(shape):
    return pl.BlockSpec(shape, lambda *i: (0,) * len(shape), pipeline_mode=pl.Buffered(1))


def norm_kernel(x_ref, g_ref, o_ref):
    for r in range(0, x_ref.shape[0], 128):
        rows = pl.ds(r, 128)
        o_ref[rows, :] = normalize(x_ref[rows, :].astype(jnp.float32), g_ref[...])


def norm(x, gain, tile, order):
    rows, width = x.shape
    return pl.pallas_call(
        norm_kernel,
        grid=(rows // tile,),
        in_specs=[pl.BlockSpec((tile, width), lambda i: (order(i), 0)), resident((1, width))],
        out_specs=pl.BlockSpec((tile, width), lambda i: (i, 0)),
        out_shape=jax.ShapeDtypeStruct((rows, width), jnp.bfloat16),
        compiler_params=params(),
        cost_estimate=cost(rows * width * 8, rows * width * 4),
        name="norm",
    )(x, gain)


def pack_kernel(plan, *refs):
    ins, outs = refs[:len(refs) - len(plan)], refs[len(refs) - len(plan):]
    for out_ref, pieces in zip(outs, plan):
        at = 0
        for n, lo, hi in pieces:
            out_ref[:, at:at + hi - lo] = ins[n][0, :, lo:hi]
            at += hi - lo


def pack(layer, parts, plan, rows, tile):
    widths = [sum(hi - lo for _, lo, hi in pieces) for pieces in plan]
    return pl.pallas_call(
        functools.partial(pack_kernel, plan),
        grid=(rows // tile,),
        in_specs=[pl.BlockSpec((1, tile, part.shape[2]), lambda i, skip=skip: (layer, i + skip // tile, 0)) for part, skip in parts],
        out_specs=[pl.BlockSpec((tile, width), lambda i: (i, 0)) for width in widths],
        out_shape=[jax.ShapeDtypeStruct((rows, width), jnp.bfloat16) for width in widths],
        compiler_params=params(),
        cost_estimate=cost(rows * sum(widths), rows * sum(widths) * 4),
        name="pack",
    )(*[part for part, _ in parts])


def attn_kernel(heads, h_ref, w_ref, cos_ref, sin_ref, o_ref, qkv_ref, vt_ref, s_ref):
    seq = h_ref.shape[0]
    half = HEAD_DIM // 2
    factor = HEAD_DIM ** -0.5 * math.log2(math.e)
    k_col = heads * HEAD_DIM
    v_col = k_col + HEAD_DIM
    tiles = seq // TILE_Q

    for c in range(0, w_ref.shape[1], 256):
        qkv_ref[:, c:c + 256] = mm(h_ref[...], w_ref[:, c:c + 256]).astype(jnp.bfloat16)

    def rotary(vals, rows):
        vals = vals.astype(jnp.float32)
        return (vals * cos_ref[rows, :] + pltpu.roll(vals, half, 1) * sin_ref[rows, :]).astype(jnp.bfloat16)

    for i in range(tiles):
        rows = pl.ds(i * TILE_Q, TILE_Q)
        qkv_ref[rows, k_col:v_col] = rotary(qkv_ref[rows, k_col:v_col], rows)
        vt_ref[:, i * TILE_Q:(i + 1) * TILE_Q] = qkv_ref[rows, v_col:v_col + HEAD_DIM].astype(jnp.float32).T.astype(jnp.bfloat16)
    key_id = lax.broadcasted_iota(jnp.int32, (TILE_Q, TILE_Q), 0)
    query_id = lax.broadcasted_iota(jnp.int32, (TILE_Q, TILE_Q), 1)
    causal = query_id >= key_id
    groups = (TILE_Q // 8, 8, TILE_Q)

    def scores(head, slot, i):
        cols = pl.ds(pl.multiple_of(head * HEAD_DIM, HEAD_DIM), HEAD_DIM)
        rows = pl.ds(i * TILE_Q, TILE_Q)
        q = rotary(qkv_ref[rows, cols], rows)
        top = None
        for j in range(i + 1):
            keys = pl.ds(j * TILE_Q, TILE_Q)
            s = lax.dot_general(qkv_ref[keys, k_col:v_col], q, (((1,), (1,)), ((), ())), preferred_element_type=jnp.float32)
            if i == j:
                s = jnp.where(causal, s, -jnp.inf)
            s_ref[slot, i, keys, :] = s
            part = jnp.max(s.reshape(groups), axis=0)
            top = part if top is None else jnp.maximum(top, part)
        return jnp.max(top, axis=0, keepdims=True)

    def powers(slot, i, top):
        total = None
        for j in range(i + 1):
            keys = pl.ds(j * TILE_Q, TILE_Q)
            e = jnp.exp2((s_ref[slot, i, keys, :] - top) * factor)
            s_ref[slot, i, keys, :] = e
            part = jnp.sum(e.reshape(groups), axis=0)
            total = part if total is None else total + part
        return 1.0 / jnp.sum(total, axis=0, keepdims=True)

    def values(head, slot, i, inverse):
        cols = pl.ds(pl.multiple_of(head * HEAD_DIM, HEAD_DIM), HEAD_DIM)
        keys = (i + 1) * TILE_Q
        p = (s_ref[slot, i, :keys, :] * inverse).astype(jnp.bfloat16)
        o_ref[pl.ds(i * TILE_Q, TILE_Q), cols] = mm(vt_ref[:, :keys], p).T.astype(jnp.bfloat16)

    @pl.loop(0, heads // SLOTS)
    def _(step):
        work = [(step * SLOTS + slot, slot, i) for slot in range(SLOTS) for i in reversed(range(tiles))]
        tops, inverses = {}, {}
        for t in range(len(work) + 2):
            if t < len(work):
                tops[t] = scores(*work[t])
            if 0 <= t - 1 < len(work):
                inverses[t - 1] = powers(*work[t - 1][1:], tops[t - 1])
            if 0 <= t - 2 < len(work):
                values(*work[t - 2], inverses[t - 2])


def attention(h, w, width, cos, sin, seq):
    tokens, depth = h.shape
    heads = width // HEAD_DIM - 2
    return pl.pallas_call(
        functools.partial(attn_kernel, heads),
        grid=(tokens // seq,),
        in_specs=[pl.BlockSpec((seq, depth), lambda b: (b, 0)), resident((depth, width)), resident(cos.shape), resident(sin.shape)],
        out_specs=pl.BlockSpec((seq, heads * HEAD_DIM), lambda b: (b, 0)),
        out_shape=jax.ShapeDtypeStruct((tokens, heads * HEAD_DIM), jnp.bfloat16),
        scratch_shapes=[
            pltpu.VMEM((seq, width), jnp.bfloat16),
            pltpu.VMEM((HEAD_DIM, seq), jnp.bfloat16),
            pltpu.VMEM((SLOTS, seq // TILE_Q, seq, TILE_Q), jnp.float32),
        ],
        compiler_params=params(),
        cost_estimate=cost(2 * tokens * depth * width + tokens * heads * seq * HEAD_DIM * 4, tokens * width * 4, tokens * heads * seq // 2),
        name="attend",
    )(h, w, cos, sin)


def out_kernel(skip, a_ref, b_ref, wa_ref, wb_ref, x_ref, g_ref, m_ref, u_ref, held_ref, sems):
    size = a_ref.shape[1] // 2
    width = m_ref.shape[1]

    @pl.when(pl.program_id(0) == 0)
    def _():
        copies = []
        for n, w_ref in enumerate((wa_ref, wb_ref)):
            for c in range(width // size):
                for k in range(2):
                    src = w_ref.at[pl.ds(c * size, size), pl.ds(skip + k * size, size)]
                    dst = held_ref.at[n, pl.ds(k * size, size), pl.ds(c * size, size)]
                    copies.append(pltpu.make_async_copy(src, dst, sems.at[len(copies)]))
        for copy in copies:
            copy.start()
        for copy in copies:
            copy.wait()

    for r in range(0, a_ref.shape[0], OUT_ROWS):
        rows = pl.ds(r, OUT_ROWS)
        acc = mm(a_ref[rows, :], held_ref[0]) + mm(b_ref[rows, :], held_ref[1])
        m = (x_ref[rows, :].astype(jnp.float32) + acc).astype(jnp.bfloat16)
        m_ref[rows, :] = m
        u_ref[rows, :] = normalize(m.astype(jnp.float32), g_ref[...])


def out_product(a, b, wa, wb, skip, x, gain, tile, order):
    tokens, depth = a.shape
    width = x.shape[1]
    lhs = pl.BlockSpec((tile, depth), lambda i: (i, 0))
    out = pl.BlockSpec((tile, width), lambda i: (i, 0))
    far = pl.BlockSpec(memory_space=pl.ANY)
    shape = jax.ShapeDtypeStruct((tokens, width), jnp.bfloat16)
    return pl.pallas_call(
        functools.partial(out_kernel, skip),
        grid=(tokens // tile,),
        in_specs=[lhs, lhs, far, far, pl.BlockSpec((tile, width), lambda i: (order(i), 0)), resident((1, width))],
        out_specs=[out, out],
        out_shape=[shape, shape],
        scratch_shapes=[pltpu.VMEM((2, depth, width), jnp.bfloat16), pltpu.SemaphoreType.DMA((8 * width // depth,))],
        compiler_params=params(),
        cost_estimate=cost(4 * tokens * depth * width, tokens * width * 10),
        name="out_product",
    )(a, b, wa, wb, x, gain)


def glu_kernel(u_ref, g_ref, v_ref, z_ref):
    for r in range(0, u_ref.shape[0], GLU_ROWS):
        rows = pl.ds(r, GLU_ROWS)
        for c in range(0, z_ref.shape[1], 128):
            cols = slice(c, c + 128)
            both = mm(u_ref[rows, :], jnp.concatenate([g_ref[:, cols], v_ref[:, cols]], axis=1))
            z_ref[rows, cols] = (jax.nn.silu(both[:, :128]) * both[:, 128:]).astype(jnp.bfloat16)


def glu(u, w):
    tokens, depth = u.shape
    width = w.shape[1] // 2
    tile, steps = 1024, width // PIECE
    return pl.pallas_call(
        glu_kernel,
        grid=(tokens // tile, steps),
        in_specs=[
            pl.BlockSpec((tile, depth), lambda i, j: (i, 0)),
            pl.BlockSpec((depth, PIECE), lambda i, j: (0, j)),
            pl.BlockSpec((depth, PIECE), lambda i, j: (0, j + steps)),
        ],
        out_specs=pl.BlockSpec((tile, PIECE), lambda i, j: (i, j)),
        out_shape=jax.ShapeDtypeStruct((tokens, width), jnp.bfloat16),
        compiler_params=params(axes=2),
        cost_estimate=cost(4 * tokens * depth * width, tokens * width * 2 + depth * width * 16, tokens * width),
        name="glu",
    )(u, w, w)


def down_kernel(more, norm_next, *refs):
    a_ref, b_ref, w_ref = refs[:3]
    out_refs, (held_ref, sems) = refs[3 + 3 * more:-2], refs[-2:]
    cut = a_ref.shape[1]
    edges = [0, 1024, cut, w_ref.shape[0]]
    spans = list(zip(edges[:-1], edges[1:]))
    copies = [pltpu.make_async_copy(w_ref.at[pl.ds(lo, hi - lo)], held_ref.at[pl.ds(lo, hi - lo)], sems.at[n]) for n, (lo, hi) in enumerate(spans)]
    blocks = [pl.ds(r, DOWN_ROWS) for r in range(0, a_ref.shape[0], DOWN_ROWS)]

    def finish(rows, acc):
        if not more:
            out_refs[0][rows, :] = acc
            return
        p_ref, m_ref, g_ref = refs[3:6]
        x = (m_ref[rows, :].astype(jnp.float32) + (p_ref[rows, :] + acc)).astype(jnp.bfloat16)
        out_refs[0][rows, :] = x
        if norm_next:
            out_refs[1][rows, :] = normalize(x.astype(jnp.float32), g_ref[...])

    @pl.when(pl.program_id(0) == 0)
    def _():
        for copy in copies:
            copy.start()
        sums = [None] * len(blocks)
        for copy, (lo, hi) in zip(copies, spans):
            copy.wait()
            for n, rows in enumerate(blocks):
                part = mm(a_ref[rows, lo:hi] if hi <= cut else b_ref[rows, lo - cut:hi - cut], held_ref[lo:hi, :])
                sums[n] = part if sums[n] is None else sums[n] + part
        for rows, acc in zip(blocks, sums):
            finish(rows, acc)

    @pl.when(pl.program_id(0) > 0)
    def _():
        for rows in blocks:
            finish(rows, mm(a_ref[rows, :], held_ref[:cut, :]) + mm(b_ref[rows, :], held_ref[cut:, :]))


def down_product(a, b, w, rest=None, last=False, order=lambda i: i):
    tokens = a.shape[0]
    depth, width = w.shape
    tile = 512
    row = lambda n: pl.BlockSpec((tile, n), lambda i: (i, 0))
    in_specs = [row(a.shape[1]), row(b.shape[1]), pl.BlockSpec(memory_space=pl.ANY)]
    more = rest is not None
    shape = jax.ShapeDtypeStruct((tokens, width), jnp.bfloat16 if more else jnp.float32)
    out_specs, out_shape = [pl.BlockSpec((tile, width), lambda i: (order(i), 0))], [shape]
    if more:
        in_specs += [row(width), row(width), resident((1, width))]
    if more and not last:
        out_specs, out_shape = out_specs + [row(width)], out_shape + [shape]
    return pl.pallas_call(
        functools.partial(down_kernel, int(more), more and not last),
        grid=(tokens // tile,),
        in_specs=in_specs,
        out_specs=out_specs,
        out_shape=out_shape,
        scratch_shapes=[pltpu.VMEM((depth, width), jnp.bfloat16), pltpu.SemaphoreType.DMA((3,))],
        compiler_params=params(),
        cost_estimate=cost(2 * tokens * depth * width, tokens * (depth * 2 + width * 8)),
        name="down_product",
    )(a, b, w, *(rest or ()))


def solution(mesh):
    act_spec = P('fsdp', 'model', None)
    col_spec = P(None, 'fsdp', 'model')
    row_spec = P(None, 'model', 'fsdp')
    swap = [(0, 1), (1, 0)]

    def gather(block, axis):
        return lax.all_gather(block, 'fsdp', axis=axis, tiled=True)

    def after(value, token):
        return lax.optimization_barrier((value, token))[0]

    def pair(own, token=None):
        own = own if token is None else after(own, token)
        return own, lax.ppermute(own, 'model', swap)

    def exchange(x):
        return lax.all_to_all(x, 'model', split_axis=0, concat_axis=0, tiled=True)

    def device_step(x_in, gain_attn, gain_mlp, rope_cos, rope_sin, w_q, w_k, w_v, w_o, w_gate, w_up, w_down):
        layers = w_q.shape[0]
        batch, part, width = x_in.shape
        seqs, seq = batch // 2, 2 * part
        cos = jnp.concatenate([rope_cos, rope_cos], axis=1)
        sin = jnp.concatenate([-rope_sin, rope_sin], axis=1)
        cut = SPLIT * PIECE
        qkv = w_q.shape[2] + w_k.shape[2] + w_v.shape[2]

        def weave(tile):
            per = part // tile

            def order(i):
                b, r = i // (2 * per), i % (2 * per)
                return (r // per) * (seqs * per) + b * per + r % per
            return order

        own = []
        mid = w_o.shape[1] // 2
        ffn = w_gate.shape[2]
        attn_parts = [(w_q, 0), (w_k, 0), (w_v, 0), (w_o, 0), (w_o, mid)]
        attn_plan = [[(n, 0, part.shape[2]) for n, (part, _) in enumerate(attn_parts)]]
        glu_plan = [[(0, 0, cut), (1, 0, cut)], [(0, cut, ffn), (1, cut, ffn)]]
        for l in range(layers):
            attn_w, = pack(l, attn_parts, attn_plan, mid, 128)
            gu_a, gu_b = pack(l, [(w_gate, 0), (w_up, 0)], glu_plan, w_gate.shape[1], 128)
            down, = pack(l, [(w_down, 0)], [[(0, 0, w_down.shape[2])]], ffn, PIECE)
            own.append((gather(attn_w, 0), gather(gu_a, 0), gather(gu_b, 0), gather(down, 1)))
        x = exchange(x_in).reshape(batch * part, width)
        h = norm(x, gain_attn[0][None], 512, weave(512))
        for l, (attn_own, a_own, b_own, d_own) in enumerate(own):
            attn_w = pair(attn_own, h)
            o0 = attention(h, attn_w[0], qkv, cos, sin, seq)
            o1 = attention(h, attn_w[1], qkv, cos, sin, seq)
            m, u = out_product(o0, o1, attn_w[0], attn_w[1], qkv, x, gain_mlp[l][None], *((512, weave(512)) if l == 0 else (1024, lambda i: i)))
            a_w = pair(a_own, u)
            za = [glu(u, a_w[0])]
            za.append(glu(after(u, za[0]), a_w[1]))
            b_w = pair(b_own, za[1])
            zb = [glu(u, b_w[0])]
            zb.append(glu(after(u, zb[0]), b_w[1]))
            d_w = pair(d_own, zb[1])
            partial = down_product(za[0], zb[0], d_w[0])[0]
            last = l + 1 == layers
            gain = gain_attn[0 if last else l + 1][None]
            out = down_product(za[1], zb[1], d_w[1], (partial, m, gain), last, weave(512) if last else lambda i: i)
            x, h = out if not last else (out[0], None)
        return exchange(x.reshape(batch, part, width))

    return jax.shard_map(device_step, mesh=mesh, in_specs=(act_spec, P(), P(), P(), P(), col_spec, col_spec, col_spec, row_spec, col_spec, col_spec, row_spec), out_specs=act_spec, check_vma=False)
```

```python
import functools
import math

import jax
import jax.numpy as jnp
from jax import lax
from jax.experimental import pallas as pl
from jax.experimental.pallas import tpu as pltpu
from jax.sharding import PartitionSpec as P

EPS = 1e-5
HEAD_DIM = 128
TILE_Q = 256
PIECE = 640
CUTS = ((2, 2, 3), (4, 3))
SLOTS = 2
GLU_ROWS = 512
OUT_ROWS = 256
VMEM_LIMIT = 62 << 20


def params(limit=VMEM_LIMIT, axes=1):
    return pltpu.CompilerParams(dimension_semantics=("arbitrary",) * axes, vmem_limit_bytes=limit)


def cost(flops, data, exps=0):
    return pl.CostEstimate(flops=flops, bytes_accessed=data, transcendentals=exps)


def mm(a, b):
    return jnp.dot(a, b, preferred_element_type=jnp.float32)


def normalize(rows, gain):
    mean_sq = jnp.mean(rows * rows, axis=-1, keepdims=True)
    return (rows * lax.rsqrt(mean_sq + EPS) * gain).astype(jnp.bfloat16)


def resident(shape):
    return pl.BlockSpec(shape, lambda *i: (0,) * len(shape), pipeline_mode=pl.Buffered(1))


def norm_kernel(x_ref, g_ref, o_ref):
    for r in range(0, x_ref.shape[0], 128):
        rows = pl.ds(r, 128)
        o_ref[rows, :] = normalize(x_ref[rows, :].astype(jnp.float32), g_ref[...])


def norm(x, gain, tile, order):
    rows, width = x.shape
    return pl.pallas_call(
        norm_kernel,
        grid=(rows // tile,),
        in_specs=[pl.BlockSpec((tile, width), lambda i: (order(i), 0)), resident((1, width))],
        out_specs=pl.BlockSpec((tile, width), lambda i: (i, 0)),
        out_shape=jax.ShapeDtypeStruct((rows, width), jnp.bfloat16),
        compiler_params=params(),
        cost_estimate=cost(rows * width * 8, rows * width * 4),
        name="norm",
    )(x, gain)


def pack_kernel(plan, *refs):
    ins, outs = refs[:len(refs) - len(plan)], refs[len(refs) - len(plan):]
    for out_ref, pieces in zip(outs, plan):
        at = 0
        for n, lo, hi in pieces:
            out_ref[:, at:at + hi - lo] = ins[n][0, :, lo:hi]
            at += hi - lo


def pack(layer, parts, plan, rows, tile):
    widths = [sum(hi - lo for _, lo, hi in pieces) for pieces in plan]
    return pl.pallas_call(
        functools.partial(pack_kernel, plan),
        grid=(rows // tile,),
        in_specs=[pl.BlockSpec((1, tile, part.shape[2]), lambda i, skip=skip: (layer, i + skip // tile, 0)) for part, skip in parts],
        out_specs=[pl.BlockSpec((tile, width), lambda i: (i, 0)) for width in widths],
        out_shape=[jax.ShapeDtypeStruct((rows, width), jnp.bfloat16) for width in widths],
        compiler_params=params(),
        cost_estimate=cost(rows * sum(widths), rows * sum(widths) * 4),
        name="pack",
    )(*[part for part, _ in parts])


def attn_kernel(heads, h_ref, w_ref, cos_ref, sin_ref, o_ref, qkv_ref, vt_ref, s_ref):
    seq = h_ref.shape[0]
    half = HEAD_DIM // 2
    factor = HEAD_DIM ** -0.5 * math.log2(math.e)
    k_col = heads * HEAD_DIM
    v_col = k_col + HEAD_DIM
    tiles = seq // TILE_Q

    for c in range(0, w_ref.shape[1], 256):
        qkv_ref[:, c:c + 256] = mm(h_ref[...], w_ref[:, c:c + 256]).astype(jnp.bfloat16)

    def rotary(vals, rows):
        vals = vals.astype(jnp.float32)
        return (vals * cos_ref[rows, :] + pltpu.roll(vals, half, 1) * sin_ref[rows, :]).astype(jnp.bfloat16)

    for i in range(tiles):
        rows = pl.ds(i * TILE_Q, TILE_Q)
        qkv_ref[rows, k_col:v_col] = rotary(qkv_ref[rows, k_col:v_col], rows)
        vt_ref[:, i * TILE_Q:(i + 1) * TILE_Q] = qkv_ref[rows, v_col:v_col + HEAD_DIM].astype(jnp.float32).T.astype(jnp.bfloat16)
    key_id = lax.broadcasted_iota(jnp.int32, (TILE_Q, TILE_Q), 0)
    query_id = lax.broadcasted_iota(jnp.int32, (TILE_Q, TILE_Q), 1)
    causal = query_id >= key_id
    groups = (TILE_Q // 8, 8, TILE_Q)

    def scores(head, slot, i):
        cols = pl.ds(pl.multiple_of(head * HEAD_DIM, HEAD_DIM), HEAD_DIM)
        rows = pl.ds(i * TILE_Q, TILE_Q)
        q = rotary(qkv_ref[rows, cols], rows)
        top = None
        for j in range(i + 1):
            keys = pl.ds(j * TILE_Q, TILE_Q)
            s = lax.dot_general(qkv_ref[keys, k_col:v_col], q, (((1,), (1,)), ((), ())), preferred_element_type=jnp.float32)
            if i == j:
                s = jnp.where(causal, s, -jnp.inf)
            s_ref[slot, i, keys, :] = s
            part = jnp.max(s.reshape(groups), axis=0)
            top = part if top is None else jnp.maximum(top, part)
        return jnp.max(top, axis=0, keepdims=True)

    def powers(slot, i, top):
        total = None
        for j in range(i + 1):
            keys = pl.ds(j * TILE_Q, TILE_Q)
            e = jnp.exp2((s_ref[slot, i, keys, :] - top) * factor)
            s_ref[slot, i, keys, :] = e
            part = jnp.sum(e.reshape(groups), axis=0)
            total = part if total is None else total + part
        return 1.0 / jnp.sum(total, axis=0, keepdims=True)

    def values(head, slot, i, inverse):
        cols = pl.ds(pl.multiple_of(head * HEAD_DIM, HEAD_DIM), HEAD_DIM)
        keys = (i + 1) * TILE_Q
        p = (s_ref[slot, i, :keys, :] * inverse).astype(jnp.bfloat16)
        o_ref[pl.ds(i * TILE_Q, TILE_Q), cols] = mm(vt_ref[:, :keys], p).T.astype(jnp.bfloat16)

    @pl.loop(0, heads // SLOTS)
    def _(step):
        work = [(step * SLOTS + slot, slot, i) for slot in range(SLOTS) for i in reversed(range(tiles))]
        tops, inverses = {}, {}
        for t in range(len(work) + 2):
            if t < len(work):
                tops[t] = scores(*work[t])
            if 0 <= t - 1 < len(work):
                inverses[t - 1] = powers(*work[t - 1][1:], tops[t - 1])
            if 0 <= t - 2 < len(work):
                values(*work[t - 2], inverses[t - 2])


def attention(h, w, width, cos, sin, seq):
    tokens, depth = h.shape
    heads = width // HEAD_DIM - 2
    return pl.pallas_call(
        functools.partial(attn_kernel, heads),
        grid=(tokens // seq,),
        in_specs=[pl.BlockSpec((seq, depth), lambda b: (b, 0)), resident((depth, width)), resident(cos.shape), resident(sin.shape)],
        out_specs=pl.BlockSpec((seq, heads * HEAD_DIM), lambda b: (b, 0)),
        out_shape=jax.ShapeDtypeStruct((tokens, heads * HEAD_DIM), jnp.bfloat16),
        scratch_shapes=[
            pltpu.VMEM((seq, width), jnp.bfloat16),
            pltpu.VMEM((HEAD_DIM, seq), jnp.bfloat16),
            pltpu.VMEM((SLOTS, seq // TILE_Q, seq, TILE_Q), jnp.float32),
        ],
        compiler_params=params(),
        cost_estimate=cost(2 * tokens * depth * width + tokens * heads * seq * HEAD_DIM * 4, tokens * width * 4, tokens * heads * seq // 2),
        name="attend",
    )(h, w, cos, sin)


def out_kernel(skip, a_ref, b_ref, wa_ref, wb_ref, x_ref, g_ref, m_ref, u_ref, held_ref, sems):
    size = a_ref.shape[1] // 2
    width = m_ref.shape[1]

    @pl.when(pl.program_id(0) == 0)
    def _():
        copies = []
        for n, w_ref in enumerate((wa_ref, wb_ref)):
            for c in range(width // size):
                for k in range(2):
                    src = w_ref.at[pl.ds(c * size, size), pl.ds(skip + k * size, size)]
                    dst = held_ref.at[n, pl.ds(k * size, size), pl.ds(c * size, size)]
                    copies.append(pltpu.make_async_copy(src, dst, sems.at[len(copies)]))
        for copy in copies:
            copy.start()
        for copy in copies:
            copy.wait()

    for r in range(0, a_ref.shape[0], OUT_ROWS):
        rows = pl.ds(r, OUT_ROWS)
        acc = mm(a_ref[rows, :], held_ref[0]) + mm(b_ref[rows, :], held_ref[1])
        m = (x_ref[rows, :].astype(jnp.float32) + acc).astype(jnp.bfloat16)
        m_ref[rows, :] = m
        u_ref[rows, :] = normalize(m.astype(jnp.float32), g_ref[...])


def out_product(a, b, wa, wb, skip, x, gain, tile, order):
    tokens, depth = a.shape
    width = x.shape[1]
    lhs = pl.BlockSpec((tile, depth), lambda i: (i, 0))
    out = pl.BlockSpec((tile, width), lambda i: (i, 0))
    far = pl.BlockSpec(memory_space=pl.ANY)
    shape = jax.ShapeDtypeStruct((tokens, width), jnp.bfloat16)
    return pl.pallas_call(
        functools.partial(out_kernel, skip),
        grid=(tokens // tile,),
        in_specs=[lhs, lhs, far, far, pl.BlockSpec((tile, width), lambda i: (order(i), 0)), resident((1, width))],
        out_specs=[out, out],
        out_shape=[shape, shape],
        scratch_shapes=[pltpu.VMEM((2, depth, width), jnp.bfloat16), pltpu.SemaphoreType.DMA((8 * width // depth,))],
        compiler_params=params(),
        cost_estimate=cost(4 * tokens * depth * width, tokens * width * 10),
        name="out_product",
    )(a, b, wa, wb, x, gain)


def glu_kernel(u_ref, g_ref, v_ref, z_ref):
    for r in range(0, u_ref.shape[0], GLU_ROWS):
        rows = pl.ds(r, GLU_ROWS)
        for c in range(0, z_ref.shape[1], 128):
            cols = slice(c, c + 128)
            both = mm(u_ref[rows, :], jnp.concatenate([g_ref[:, cols], v_ref[:, cols]], axis=1))
            z_ref[rows, cols] = (jax.nn.silu(both[:, :128]) * both[:, 128:]).astype(jnp.bfloat16)


def glu(u, w):
    tokens, depth = u.shape
    width = w.shape[1] // 2
    tile, steps = 1024, width // PIECE
    return pl.pallas_call(
        glu_kernel,
        grid=(tokens // tile, steps),
        in_specs=[
            pl.BlockSpec((tile, depth), lambda i, j: (i, 0)),
            pl.BlockSpec((depth, PIECE), lambda i, j: (0, j)),
            pl.BlockSpec((depth, PIECE), lambda i, j: (0, j + steps)),
        ],
        out_specs=pl.BlockSpec((tile, PIECE), lambda i, j: (i, j)),
        out_shape=jax.ShapeDtypeStruct((tokens, width), jnp.bfloat16),
        compiler_params=params(axes=2),
        cost_estimate=cost(4 * tokens * depth * width, tokens * width * 2 + depth * width * 16, tokens * width),
        name="glu",
    )(u, w, w)


def down_kernel(count, more, norm_next, core_ref, *refs):
    z_refs, w_ref, refs = refs[:count], refs[count], refs[count + 1:]
    acc, at = None, 0
    for z_ref in z_refs:
        part = mm(z_ref[...], w_ref[at:at + z_ref.shape[1], :])
        acc = part if acc is None else acc + part
        at += z_ref.shape[1]
    if not more:
        refs[0][...] = acc
        return
    p_ref, m_ref, g_ref, x_ref = refs[:4]
    x = (m_ref[...].astype(jnp.float32) + (p_ref[...] + acc)).astype(jnp.bfloat16)
    x_ref[...] = x
    if norm_next:
        refs[4][...] = normalize(x.astype(jnp.float32), g_ref[...])


def down_product(core, zs, w, rest=None, norm_next=False, pick=lambda i, core: i, place=lambda i, core: i, share=1, rows=None):
    tokens = zs[0].shape[0]
    depth, width = w.shape
    tile = 256
    row = lambda n, at=pick: pl.BlockSpec((tile, n), lambda i, core: (at(i, core[0]), 0))
    more = rest is not None
    shape = jax.ShapeDtypeStruct((rows or tokens, width), jnp.bfloat16 if more else jnp.float32)
    in_specs = [row(z.shape[1]) for z in zs] + [resident(w.shape)]
    if more:
        in_specs += [row(width), row(width), resident((1, width))]
    outs = 2 if norm_next else 1
    return pl.pallas_call(
        functools.partial(down_kernel, len(zs), more, norm_next),
        grid_spec=pltpu.PrefetchScalarGridSpec(
            num_scalar_prefetch=1,
            grid=(tokens // tile // share,),
            in_specs=in_specs,
            out_specs=[row(width, place)] * outs,
        ),
        out_shape=[shape] * outs,
        compiler_params=params(),
        cost_estimate=cost(2 * tokens * depth * width // share, tokens * (depth * 2 + width * 8) // share),
        name="down_product",
    )(core, *zs, w, *(rest or ()))


def solution(mesh):
    act_spec = P('fsdp', 'model', None)
    col_spec = P(None, 'fsdp', 'model')
    row_spec = P(None, 'model', 'fsdp')
    swap = [(0, 1), (1, 0)]

    def gather(block, axis):
        return lax.all_gather(block, 'fsdp', axis=axis, tiled=True)

    def after(value, token):
        return lax.optimization_barrier((value, token))[0]

    def pair(own, token=None):
        own = own if token is None else after(own, token)
        return own, lax.ppermute(own, 'model', swap)

    def exchange(x):
        return lax.all_to_all(x, 'model', split_axis=0, concat_axis=0, tiled=True)

    def device_step(x_in, gain_attn, gain_mlp, rope_cos, rope_sin, w_q, w_k, w_v, w_o, w_gate, w_up, w_down):
        layers = w_q.shape[0]
        core = lax.axis_index('model')[None]
        batch, part, width = x_in.shape
        seqs, seq = batch // 2, 2 * part
        cos = jnp.concatenate([rope_cos, rope_cos], axis=1)
        sin = jnp.concatenate([-rope_sin, rope_sin], axis=1)
        qkv = w_q.shape[2] + w_k.shape[2] + w_v.shape[2]

        def weave(tile):
            per = part // tile

            def order(i):
                b, r = i // (2 * per), i % (2 * per)
                return (r // per) * (seqs * per) + b * per + r % per
            return order

        own = []
        mid = w_o.shape[1] // 2
        ffn = w_gate.shape[2]
        attn_parts = [(w_q, 0), (w_k, 0), (w_v, 0), (w_o, 0), (w_o, mid)]
        attn_plan = [[(n, 0, part.shape[2]) for n, (part, _) in enumerate(attn_parts)]]
        for l in range(layers):
            attn_w, = pack(l, attn_parts, attn_plan, mid, 128)
            edges = [PIECE * sum(CUTS[l > 0][:n]) for n in range(len(CUTS[l > 0]) + 1)]
            glu_plan = [[(0, lo, hi), (1, lo, hi)] for lo, hi in zip(edges[:-1], edges[1:])]
            gated = pack(l, [(w_gate, 0), (w_up, 0)], glu_plan, w_gate.shape[1], 128)
            down, = pack(l, [(w_down, 0)], [[(0, 0, w_down.shape[2])]], ffn, PIECE)
            own.append((gather(attn_w, 0), [gather(w, 0) for w in gated], gather(down, 1)))
        x = exchange(x_in).reshape(batch * part, width)
        h = norm(x, gain_attn[0][None], 512, weave(512))
        for l, (attn_own, glu_own, d_own) in enumerate(own):
            attn_w = pair(attn_own, h)
            o0 = attention(h, attn_w[0], qkv, cos, sin, seq)
            o1 = attention(h, attn_w[1], qkv, cos, sin, seq)
            m, u = out_product(o0, o1, attn_w[0], attn_w[1], qkv, x, gain_mlp[l][None], 512, weave(512) if l == 0 else lambda i: i)
            mine, other, token = [], [], u
            for w in glu_own:
                w = pair(w, token)
                mine.append(glu(after(u, token), w[0]))
                token = glu(after(u, mine[-1]), w[1])
                other.append(token)
            d_w = pair(d_own, token)
            partial = down_product(core, mine, d_w[0])[0]
            if l + 1 < layers:
                x, h = down_product(core, other, d_w[1], (partial, m, gain_attn[l + 1][None]), True)
        rest = (partial, m, gain_attn[0][None])
        per = part // 256

        def half(flip, offset):
            def pick(i, c):
                return i // per * (2 * per) + (1 - c if flip else c) * per + i % per

            def place(i, c):
                return i + (c * (seqs * per) if offset else 0)
            return pick, place

        sent = down_product(core, other, d_w[1], rest, False, *half(True, False), share=2, rows=batch * part // 2)[0]
        got = lax.ppermute(sent, 'model', swap)
        kept = down_product(core, [after(other[0], sent), *other[1:]], d_w[1], rest, False, *half(False, True), share=2)[0]
        y = lax.dynamic_update_slice(kept, got, ((1 - core[0]) * (seqs * part), 0))
        return y.reshape(batch, part, width)

    return jax.shard_map(device_step, mesh=mesh, in_specs=(act_spec, P(), P(), P(), P(), col_spec, col_spec, col_spec, row_spec, col_spec, col_spec, row_spec), out_specs=act_spec, check_vma=False)
```
